32 devices in a mesh: act: 4 (over y, x), virt: 8 (over z, core).
Axes of the slice: x: 2, y: 2, z: 4, core: 2. Of those that a mesh axis runs over, the one named last changes fastest.
Arguments:
- amplitudes: bfloat16 [400, 640, 640], P('act', 'virt'), may hold values from -6 to 6
- virtual_fock_block: bfloat16 [640, 640], replicated, may hold values from -1 to 3.1, as said below
- metric: bfloat16 [400, 400], replicated, may hold values from -3.5 to 3.5, as said below
- active_block: bfloat16 [400, 400], replicated, may hold values from -0.3125 to 0.3125
Outputs:
- residual_vec: bfloat16 [400, 640, 640], P('act', 'virt')
- rayleigh: float32 [], replicated
- res_norm: float32 [], replicated
The draws below stay inside these ranges and needn't reach their ends.
Inputs may be any that keep to these rules, and one draw needn't show every extreme that they name: `virtual_fock_block`: symmetric. `metric`: symmetric positive definite.
All inputs are finite; a program needn't handle non-finite values.
Results may differ from the reference program's by a relative error of at most 0.0099.
Values may be sent and summed in bfloat16 or wider, within the bound.
A program may use at most 192 MiB of HBM per device.

```python
import jax
import jax.numpy as jnp
from jax import lax

NV = 640
TU = 400


def draw_virtual_fock_block(key, part):
    leading_key, second_key = jax.random.split(jax.random.fold_in(key, 11))
    energies = jax.random.uniform(leading_key, (NV,), jnp.float32, 0.5, 3.0)
    coupling = jax.random.uniform(second_key, (NV, NV), jnp.float32, -1.0, 1.0) * 1.7
    coupling = (coupling + coupling.T) * (0.35 / math_sqrt(NV))
    coupling = coupling * (1.0 - jnp.eye(NV, dtype=jnp.float32))
    return (jnp.diag(energies) + coupling).astype(jnp.bfloat16)


def math_sqrt(value):
    return float(value) ** 0.5


def draw_metric(key, part):
    leading_key = jax.random.fold_in(jax.random.fold_in(key, 23), 0)
    factor = jax.random.uniform(leading_key, (TU, TU), jnp.float32, -1.7, 1.7)
    product = jnp.dot(factor, factor.T, precision=lax.Precision.HIGHEST) / TU
    return (0.5 * jnp.eye(TU, dtype=jnp.float32) + product).astype(jnp.bfloat16)


def level_of(own_key, extent, pieces, least, top_value):
    level, own = 1.0, jax.random.fold_in(own_key, 6)
    for axis_at, shards_of in pieces:
        heights = jnp.exp(jax.random.uniform(jax.random.fold_in(own, axis_at), (shards_of,), jnp.float32, least / len(pieces), top_value / len(pieces)))
        level = level * jnp.repeat(heights, extent[axis_at] // shards_of).reshape([-1 if axis == axis_at else 1 for axis in range(len(extent))])
    return level


def noise(key, shape, scale, most, shards=(), held_as=jnp.bfloat16):
    drawn = jax.random.normal(key, shape, jnp.float32) * scale
    if len(shards) > 0:
        drawn = level_of(key, shape, shards, -0.22, 0.18) * drawn
    return jnp.clip(drawn, min=-most, max=most).astype(held_as)


def setup_inputs(seed: int = 0) -> dict:
    keys = jax.random.split(jax.random.key(seed), 5)
    amplitudes = noise(keys[0], (TU, NV, NV), 1.0, 6.0, ((0, 4), (1, 8)))
    virtual_fock_block = draw_virtual_fock_block(jax.random.fold_in(keys[4], 71), 0)
    metric = draw_metric(jax.random.fold_in(keys[4], 71), 0)
    active_block = noise(keys[3], (TU, TU), TU ** -0.5, 0.3125)
    return dict(amplitudes=amplitudes, virtual_fock_block=virtual_fock_block, metric=metric, active_block=active_block)


def reference(amplitudes, virtual_fock_block, metric, active_block):
    broadened_fock = virtual_fock_block.astype(jnp.float32)
    block_of_rows = 32
    blocks_count = NV // block_of_rows
    indices = jnp.arange(blocks_count, dtype=jnp.int32)

    def metric_rows(index):
        start = (index * block_of_rows).astype(jnp.int32)
        trial_rows = lax.dynamic_slice_in_dim(amplitudes, start, block_of_rows, 1)
        flat_trial = trial_rows.reshape(TU, block_of_rows * NV)
        weighted_rows = jnp.dot(metric, flat_trial, preferred_element_type=jnp.float32)
        return weighted_rows.astype(jnp.bfloat16).reshape(TU, block_of_rows, NV)

    half_blocks = lax.map(metric_rows, indices)
    weighted_half = jnp.moveaxis(half_blocks, 0, 1).reshape(TU, NV, NV)

    def left_group(group_rows):
        return jnp.einsum("ac,tcb->tab", broadened_fock, group_rows.astype(jnp.float32)).astype(jnp.bfloat16)

    left_portion = lax.map(left_group, weighted_half.reshape(TU // 4, 4, NV, NV)).reshape(TU, NV, NV)

    def project(index):
        start = (index * block_of_rows).astype(jnp.int32)
        trial_rows = lax.dynamic_slice_in_dim(amplitudes, start, block_of_rows, 1)
        halved_rows = lax.dynamic_slice_in_dim(weighted_half, start, block_of_rows, 1)
        left_rows = lax.dynamic_slice_in_dim(left_portion, start, block_of_rows, 1)
        flat_trial = trial_rows.reshape(TU, block_of_rows * NV)
        rightside_rows = jnp.einsum("wuv,vq->wuq", halved_rows.astype(jnp.float32), broadened_fock)
        sigma_rows = left_rows.astype(jnp.float32).reshape(TU, block_of_rows * NV) + rightside_rows.reshape(TU, block_of_rows * NV) + jnp.dot(active_block, flat_trial, preferred_element_type=jnp.float32)
        weighted_rows = jnp.dot(metric, flat_trial, preferred_element_type=jnp.float32)
        return sigma_rows, weighted_rows, flat_trial.astype(jnp.float32)

    def intersect(index):
        sigma_rows, weighted_rows, trial_wide = project(index)
        return jnp.sum(trial_wide * sigma_rows), jnp.sum(trial_wide * weighted_rows)

    numer_parts, denom_parts = lax.map(intersect, indices)
    numerator = jnp.sum(numer_parts)
    denominator = jnp.sum(denom_parts)
    rayleigh = numerator / denominator

    def finish(index):
        sigma_rows, weighted_rows, trial_wide = project(index)
        resid = sigma_rows - rayleigh * weighted_rows
        return resid.astype(jnp.bfloat16).reshape(TU, block_of_rows, NV), jnp.sum(resid * resid)

    resid_blocks, square_parts = lax.map(finish, indices)
    residual_vec = jnp.moveaxis(resid_blocks, 0, 1).reshape(TU, NV, NV)
    res_norm = jnp.sum(square_parts) / denominator
    return residual_vec, rayleigh, res_norm
```

```python
import functools

import jax
import jax.numpy as jnp
from jax import lax
from jax.experimental import pallas as pl
from jax.experimental.pallas import tpu as pltpu
from jax.sharding import PartitionSpec as P

MESH = pl.DeviceIdType.MESH
AHEAD = 4


def left_kernel(peers, pair_count, fock_ref, image_ref, out_ref, held, made, sent, landed, back_sent, back_landed):
    group = lax.axis_index("act")
    me = lax.axis_index("virt")
    rounds = held.shape[0]
    barrier = pltpu.get_barrier_semaphore()
    for peer in range(peers):

        @pl.when(peer != me)
        def _():
            pl.semaphore_signal(barrier, inc=1, device_id=(group, peer), device_id_type=MESH)

    pl.semaphore_wait(barrier, peers - 1)

    def forward(r, peer):
        return pltpu.make_async_remote_copy(
            src_ref=image_ref.at[r * peers + peer], dst_ref=held.at[r, me],
            send_sem=sent.at[r, peer], recv_sem=landed.at[r, me],
            device_id=(group, peer), device_id_type=MESH)

    def forward_own(r):
        return pltpu.make_async_copy(image_ref.at[r * peers + me], held.at[r, me], landed.at[r, me])

    def backward(r, peer):
        return pltpu.make_async_remote_copy(
            src_ref=made.at[r, peer], dst_ref=out_ref.at[r * peers + me],
            send_sem=back_sent.at[r, peer], recv_sem=back_landed.at[r, me],
            device_id=(group, peer), device_id_type=MESH)

    def backward_own(r):
        return pltpu.make_async_copy(made.at[r, me], out_ref.at[r * peers + me], back_landed.at[r, me])

    def arrival(r, peer):
        return pltpu.make_async_remote_copy(
            src_ref=made.at[r, peer], dst_ref=held.at[r, peer],
            send_sem=sent.at[r, peer], recv_sem=landed.at[r, peer],
            device_id=(group, peer), device_id_type=MESH)

    def back_arrival(r, peer):
        return pltpu.make_async_remote_copy(
            src_ref=made.at[r, peer], dst_ref=out_ref.at[r * peers + peer],
            send_sem=back_sent.at[r, peer], recv_sem=back_landed.at[r, peer],
            device_id=(group, peer), device_id_type=MESH)

    def launch(r):
        for step in range(peers):
            peer = lax.rem(me + step, peers)

            @pl.when(r * peers + peer < pair_count)
            def _(step=step, peer=peer):
                if step == 0:
                    forward_own(r).start()
                else:
                    forward(r, peer).start()

    for r in range(min(AHEAD, rounds)):
        launch(r)

    def body(r, carry):
        @pl.when(r + AHEAD < rounds)
        def _():
            launch(r + AHEAD)

        @pl.when(r * peers + me < pair_count)
        def _():
            forward_own(r).wait()
            for step in range(1, peers):
                arrival(r, lax.rem(me + step, peers)).wait_recv()
            rows, width = held.shape[2], held.shape[3]
            block = held[r].reshape(peers * rows, width)
            product = jnp.dot(fock_ref[...], block, preferred_element_type=jnp.float32)
            made[r] = product.astype(jnp.bfloat16).reshape(peers, rows, width)
            backward_own(r).start()
            for step in range(1, peers):
                backward(r, lax.rem(me + step, peers)).start()

        return carry

    lax.fori_loop(0, rounds, body, 0)

    def drain(r, carry):
        mine = r * peers + me < pair_count

        @pl.when(mine)
        def _():
            backward_own(r).wait()

        for step in range(1, peers):
            peer = lax.rem(me + step, peers)

            @pl.when(r * peers + peer < pair_count)
            def _(peer=peer):
                forward(r, peer).wait_send()
                back_arrival(r, peer).wait_recv()

            @pl.when(mine)
            def _(peer=peer):
                backward(r, peer).wait_send()

        return carry

    lax.fori_loop(0, rounds, drain, 0)


def apply_left(image, fock, peers):
    pairs, rows, width = image.shape
    padded = -(-rows // 16) * 16
    if padded != rows:
        image = jnp.pad(image, ((0, 0), (0, padded - rows), (0, 0)))
        spread = jnp.pad(
            fock.reshape(peers, rows, peers, rows),
            ((0, 0), (0, padded - rows), (0, 0), (0, padded - rows)))
        fock = spread.reshape(peers * padded, peers * padded)
    rounds = -(-pairs // peers)
    out = pl.pallas_call(
        functools.partial(left_kernel, peers, pairs),
        out_shape=jax.ShapeDtypeStruct(image.shape, jnp.bfloat16),
        in_specs=[pl.BlockSpec(memory_space=pltpu.VMEM), pl.BlockSpec(memory_space=pl.ANY)],
        out_specs=pl.BlockSpec(memory_space=pl.ANY),
        scratch_shapes=[
            pltpu.VMEM((rounds, peers, padded, width), jnp.bfloat16),
            pltpu.VMEM((rounds, peers, padded, width), jnp.bfloat16),
            pltpu.SemaphoreType.DMA((rounds, peers)),
            pltpu.SemaphoreType.DMA((rounds, peers)),
            pltpu.SemaphoreType.DMA((rounds, peers)),
            pltpu.SemaphoreType.DMA((rounds, peers)),
        ],
        compiler_params=pltpu.CompilerParams(
            collective_id=0, has_side_effects=True, vmem_limit_bytes=48 * 2**20),
        cost_estimate=pl.CostEstimate(
            flops=2 * pairs * rows * rows * peers * width, bytes_accessed=800 * 2**20, transcendentals=0),
    )(fock, image)
    return out[:, :rows, :]


def local(amplitudes, virtual_fock_block, metric, active_block):
    pairs, rows, width = amplitudes.shape
    peers = lax.axis_size("virt")
    trial = lax.all_to_all(amplitudes, "act", split_axis=1, concat_axis=0, tiled=True)
    flat = trial.reshape(trial.shape[0], -1)
    weighted_flat = jnp.dot(metric, flat, preferred_element_type=jnp.float32).astype(jnp.bfloat16)
    active_flat = jnp.dot(active_block, flat, preferred_element_type=jnp.float32).astype(jnp.bfloat16)
    weighted = lax.all_to_all(weighted_flat.reshape(trial.shape), "act", split_axis=0, concat_axis=1, tiled=True)
    active = lax.all_to_all(active_flat.reshape(trial.shape), "act", split_axis=0, concat_axis=1, tiled=True)
    left = apply_left(weighted, virtual_fock_block, peers)
    right = jnp.einsum("tac,cb->tab", weighted, virtual_fock_block, preferred_element_type=jnp.float32)
    sigma = left.astype(jnp.float32) + right + active.astype(jnp.float32)
    wide = amplitudes.astype(jnp.float32)
    numer_local = jnp.sum(wide * sigma)
    denom_local = jnp.sum(wide * weighted.astype(jnp.float32))
    numerator, denominator = lax.psum((numer_local, denom_local), ("act", "virt"))
    rayleigh = numerator / denominator
    resid = sigma - rayleigh * weighted.astype(jnp.float32)
    squares = lax.psum(jnp.sum(resid * resid), ("act", "virt"))
    return resid.astype(jnp.bfloat16), rayleigh, squares / denominator


def solution(mesh):
    placed = (P("act", "virt", None), P(), P(), P())
    return jax.shard_map(
        local,
        mesh=mesh,
        in_specs=placed,
        out_specs=(P("act", "virt", None), P(), P()),
        check_vma=False,
    )
```

```python
import functools

import jax
import jax.numpy as jnp
from jax import lax
from jax.experimental import pallas as pl
from jax.experimental.pallas import tpu as pltpu
from jax.sharding import PartitionSpec as P

MESH = pl.DeviceIdType.MESH
AHEAD = 4


def stage_kernel(first, peers, groups, pair_count, start, *refs):
    if first:
        (shift_ref, fock_ref, metric_ref, active_ref, image_ref, rows_ref,
         left_ref, back_ref, kept_ref) = refs[:9]
        scratch = refs[9:]
    else:
        fock_ref, metric_ref, kept_ref, image_ref, rows_ref, left_ref, back_ref = refs[:7]
        scratch = refs[7:]
    (held, made, row_held, row_made, sent, landed, back_sent, back_landed,
     row_sent, row_landed, row_back_sent, row_back_landed) = scratch
    group = lax.axis_index("act")
    me = lax.axis_index("virt")
    rounds, rows, width = held.shape[0], held.shape[2], held.shape[3]
    items = row_held.shape[0]
    per_step = -(-items // rounds)
    barrier = pltpu.get_barrier_semaphore()
    for step in range(1, peers):
        pl.semaphore_signal(
            barrier, inc=1, device_id=(group, lax.rem(me + step, peers)), device_id_type=MESH)
    for step in range(1, groups):
        pl.semaphore_signal(
            barrier, inc=1, device_id=(lax.rem(group + step, groups), me), device_id_type=MESH)
    pl.semaphore_wait(barrier, peers + groups - 2)

    def slab(t):
        return image_ref.at[t, :, pl.ds(start, width)]

    def forward(r, peer):
        return pltpu.make_async_remote_copy(
            src_ref=slab(r * peers + peer), dst_ref=held.at[r, me],
            send_sem=sent.at[r, peer], recv_sem=landed.at[r, me],
            device_id=(group, peer), device_id_type=MESH)

    def forward_own(r):
        return pltpu.make_async_copy(slab(r * peers + me), held.at[r, me], landed.at[r, me])

    def arrival(r, peer):
        return pltpu.make_async_remote_copy(
            src_ref=made.at[r, peer], dst_ref=held.at[r, peer],
            send_sem=sent.at[r, peer], recv_sem=landed.at[r, peer],
            device_id=(group, peer), device_id_type=MESH)

    def backward(r, peer):
        return pltpu.make_async_remote_copy(
            src_ref=made.at[r, peer], dst_ref=left_ref.at[r * peers + me],
            send_sem=back_sent.at[r, peer], recv_sem=back_landed.at[r, me],
            device_id=(group, peer), device_id_type=MESH)

    def backward_own(r):
        return pltpu.make_async_copy(made.at[r, me], left_ref.at[r * peers + me], back_landed.at[r, me])

    def back_arrival(r, peer):
        return pltpu.make_async_remote_copy(
            src_ref=made.at[r, peer], dst_ref=left_ref.at[r * peers + peer],
            send_sem=back_sent.at[r, peer], recv_sem=back_landed.at[r, peer],
            device_id=(group, peer), device_id_type=MESH)

    def row_forward(i, peer):
        return pltpu.make_async_remote_copy(
            src_ref=rows_ref.at[peer * items + i], dst_ref=row_held.at[i, group],
            send_sem=row_sent.at[i, peer], recv_sem=row_landed.at[i, group],
            device_id=(peer, me), device_id_type=MESH)

    def row_forward_own(i):
        return pltpu.make_async_copy(
            rows_ref.at[group * items + i], row_held.at[i, group], row_landed.at[i, group])

    def row_arrival(i, peer):
        return pltpu.make_async_remote_copy(
            src_ref=rows_ref.at[peer * items + i], dst_ref=row_held.at[i, peer],
            send_sem=row_sent.at[i, peer], recv_sem=row_landed.at[i, peer],
            device_id=(peer, me), device_id_type=MESH)

    def row_backward(i, peer):
        return pltpu.make_async_remote_copy(
            src_ref=row_made.at[i, peer], dst_ref=back_ref.at[group * items + i],
            send_sem=row_back_sent.at[i, peer], recv_sem=row_back_landed.at[i, group],
            device_id=(peer, me), device_id_type=MESH)

    def row_backward_own(i):
        return pltpu.make_async_copy(
            row_made.at[i, group], back_ref.at[group * items + i], row_back_landed.at[i, group])

    def row_back_arrival(i, peer):
        return pltpu.make_async_remote_copy(
            src_ref=row_made.at[i, peer], dst_ref=back_ref.at[peer * items + i],
            send_sem=row_back_sent.at[i, peer], recv_sem=row_back_landed.at[i, peer],
            device_id=(peer, me), device_id_type=MESH)

    def launch(r):
        for step in range(peers):
            peer = lax.rem(me + step, peers)

            @pl.when(r * peers + peer < pair_count)
            def _(step=step, peer=peer):
                if step == 0:
                    forward_own(r).start()
                else:
                    forward(r, peer).start()

        def launch_row(i, carry):
            row_forward_own(i).start()
            for step in range(1, groups):
                row_forward(i, lax.rem(group + step, groups)).start()
            return carry

        lax.fori_loop(jnp.minimum(r * per_step, items), jnp.minimum((r + 1) * per_step, items), launch_row, 0)

    def ahead(r, carry):
        launch(r)
        return carry

    lax.fori_loop(0, min(AHEAD, rounds), ahead, 0)

    def mix(matrix_ref, i):
        total = jnp.dot(matrix_ref[0], row_held[i, 0], preferred_element_type=jnp.float32)
        for q in range(1, groups):
            total += jnp.dot(matrix_ref[q], row_held[i, q], preferred_element_type=jnp.float32)
        return total

    def mix_row(i, carry):
        row_forward_own(i).wait()
        for step in range(1, groups):
            row_arrival(i, lax.rem(group + step, groups)).wait_recv()
        tall = row_held.shape[2]
        weighted = mix(metric_ref, i)
        if first:
            half = weighted.astype(jnp.bfloat16)
            row_made[i] = half.reshape(groups, tall, -1)
            active = mix(active_ref, i) - shift_ref[0] * (weighted - half.astype(jnp.float32))
            kept_ref[i] = active.astype(jnp.bfloat16).reshape(groups, tall, -1)
        else:
            wide = row_held.shape[3]
            kept = kept_ref[i, :, :, :wide].astype(jnp.float32)
            row_made[i, :, :, :wide] = (kept + weighted.reshape(groups, tall, wide)).astype(jnp.bfloat16)
            row_made[i, :, :, wide:] = kept_ref[i, :, :, wide:]
        row_backward_own(i).start()
        for step in range(1, groups):
            row_backward(i, lax.rem(group + step, groups)).start()
        return carry

    def body(r, carry):
        @pl.when(r + AHEAD < rounds)
        def _():
            launch(r + AHEAD)

        lax.fori_loop(jnp.minimum(r * per_step, items), jnp.minimum((r + 1) * per_step, items), mix_row, 0)

        @pl.when(r * peers + me < pair_count)
        def _():
            forward_own(r).wait()
            for step in range(1, peers):
                arrival(r, lax.rem(me + step, peers)).wait_recv()
            block = held[r].reshape(peers * rows, width)
            product = jnp.dot(fock_ref[...], block, preferred_element_type=jnp.float32)
            made[r] = product.astype(jnp.bfloat16).reshape(peers, rows, width)
            backward_own(r).start()
            for step in range(1, peers):
                backward(r, lax.rem(me + step, peers)).start()

        return carry

    lax.fori_loop(0, rounds, body, 0)

    def drain(r, carry):
        mine = r * peers + me < pair_count

        @pl.when(mine)
        def _():
            backward_own(r).wait()

        for step in range(1, peers):
            peer = lax.rem(me + step, peers)

            @pl.when(r * peers + peer < pair_count)
            def _(peer=peer):
                forward(r, peer).wait_send()
                back_arrival(r, peer).wait_recv()

            @pl.when(mine)
            def _(peer=peer):
                backward(r, peer).wait_send()

        return carry

    lax.fori_loop(0, rounds, drain, 0)

    def drain_row(i, carry):
        row_backward_own(i).wait()
        for step in range(1, groups):
            peer = lax.rem(group + step, groups)
            row_forward(i, peer).wait_send()
            row_back_arrival(i, peer).wait_recv()
            row_backward(i, peer).wait_send()
        return carry

    lax.fori_loop(0, items, drain_row, 0)


def stage(first, peers, groups, pairs, start, width, smalls, kept, image, turned):
    fock = smalls[1] if first else smalls[0]
    padded = image.shape[1]
    count, tall, row_width = turned.shape
    items = count // groups
    rounds = -(-pairs // peers)
    full = image.shape[2]
    whole = pl.BlockSpec(memory_space=pltpu.VMEM)
    anywhere = pl.BlockSpec(memory_space=pl.ANY)
    made_rows = (items, groups, tall, full)
    out_shape = [
        jax.ShapeDtypeStruct((pairs, padded, width), jnp.bfloat16),
        jax.ShapeDtypeStruct((count, tall, full), jnp.bfloat16),
    ]
    out_specs = [anywhere, anywhere]
    if first:
        in_specs = [pl.BlockSpec(memory_space=pltpu.SMEM)] + [whole] * 3
        out_shape.append(jax.ShapeDtypeStruct(made_rows, jnp.bfloat16))
        out_specs.append(whole)
        operands = smalls
    else:
        in_specs = [whole] * 3
        operands = (*smalls, kept)
    dma = pltpu.SemaphoreType.DMA
    return pl.pallas_call(
        functools.partial(stage_kernel, first, peers, groups, pairs, start),
        out_shape=out_shape,
        in_specs=in_specs + [anywhere] * 2,
        out_specs=out_specs,
        scratch_shapes=[
            pltpu.VMEM((rounds, peers, padded, width), jnp.bfloat16),
            pltpu.VMEM((rounds, peers, padded, width), jnp.bfloat16),
            pltpu.VMEM((items, groups, tall, row_width), jnp.bfloat16),
            pltpu.VMEM(made_rows, jnp.bfloat16),
            dma((rounds, peers)), dma((rounds, peers)), dma((rounds, peers)), dma((rounds, peers)),
            dma((items, groups)), dma((items, groups)), dma((items, groups)), dma((items, groups)),
        ],
        compiler_params=pltpu.CompilerParams(
            collective_id=1 if first else 2, has_side_effects=True, vmem_limit_bytes=60 * 2**20),
        cost_estimate=pl.CostEstimate(
            flops=2 * pairs * fock.size * width, bytes_accessed=400 * 2**20, transcendentals=0),
    )(*operands, image, turned)


def sum_kernel(groups, peers, part_ref, total_ref, slots, sent, landed):
    group, me = lax.axis_index("act"), lax.axis_index("virt")
    count = groups * peers
    mine = group * peers + me
    barrier = pltpu.get_barrier_semaphore()

    def target(step):
        other = lax.rem(mine + step, count)
        return other, (other // peers, lax.rem(other, peers))

    def greet(step, carry):
        pl.semaphore_signal(barrier, inc=1, device_id=target(step)[1], device_id_type=MESH)
        return carry

    lax.fori_loop(1, count, greet, 0)
    pl.semaphore_wait(barrier, count - 1)

    def copy(step, slot):
        other, place = target(step)
        return pltpu.make_async_remote_copy(
            src_ref=part_ref, dst_ref=slots.at[slot], send_sem=sent.at[other], recv_sem=landed.at[slot],
            device_id=place, device_id_type=MESH)

    def send(step, carry):
        copy(step, mine).start()
        return carry

    lax.fori_loop(1, count, send, 0)
    slots[mine] = part_ref[...]

    def receive(step, carry):
        copy(step, target(step)[0]).wait_recv()
        return carry

    lax.fori_loop(1, count, receive, 0)
    total_ref[...] = jnp.sum(slots[...], axis=0)

    def finish(step, carry):
        copy(step, mine).wait_send()
        return carry

    lax.fori_loop(1, count, finish, 0)


def sum_all(values, groups, peers, number):
    part = jnp.zeros((8, 128), jnp.float32)
    for at, value in enumerate(values):
        part = part.at[at].set(value)
    total = pl.pallas_call(
        functools.partial(sum_kernel, groups, peers),
        out_shape=jax.ShapeDtypeStruct(part.shape, jnp.float32),
        in_specs=[pl.BlockSpec(memory_space=pltpu.VMEM)],
        out_specs=pl.BlockSpec(memory_space=pltpu.VMEM),
        scratch_shapes=[
            pltpu.VMEM((groups * peers, *part.shape), jnp.float32),
            pltpu.SemaphoreType.DMA((groups * peers,)),
            pltpu.SemaphoreType.DMA((groups * peers,)),
        ],
        compiler_params=pltpu.CompilerParams(collective_id=number, has_side_effects=True),
    )(part)
    return [total[at, 0] for at in range(len(values))]


def local(amplitudes, virtual_fock_block, metric, active_block):
    pairs, rows, width = amplitudes.shape
    peers, groups = lax.axis_size("virt"), lax.axis_size("act")
    fock = virtual_fock_block
    padded = -(-rows // 16) * 16
    tall = -(-pairs // 8) * 8
    cut = (3 * width // 5) // 128 * 128

    def widen(array):
        if padded == rows:
            return array
        return jnp.pad(array, ((0, 0), (0, padded - rows), (0, 0)))

    def turn(array):
        return jnp.pad(jnp.transpose(array, (1, 0, 2)), ((0, 0), (0, tall - pairs), (0, 0)))

    def turn_back(array):
        return jnp.transpose(array, (1, 0, 2))[:pairs]

    def pair_matrix(array):
        room = tall - pairs
        spread = jnp.pad(
            array.reshape(groups, pairs, groups, pairs), ((0, 0), (0, room), (0, 0), (0, room)))
        return jnp.transpose(spread, (2, 0, 1, 3)).reshape(groups, groups * tall, tall)

    spread = fock
    if padded != rows:
        room = padded - rows
        spread = jnp.pad(
            fock.reshape(peers, rows, peers, rows), ((0, 0), (0, room), (0, 0), (0, room))
        ).reshape(peers * padded, peers * padded)
    metric_parts, active_parts = pair_matrix(metric), pair_matrix(active_block)
    shift = (2.0 / fock.shape[0]) * jnp.sum(jnp.diagonal(fock).astype(jnp.float32))
    applied, weighted_turned, kept = stage(
        True, peers, groups, pairs, 0, cut, (shift.reshape(1), spread, metric_parts, active_parts),
        None, widen(amplitudes), turn(amplitudes))
    weighted = turn_back(weighted_turned)
    left, rest_turned = stage(
        False, peers, groups, pairs, cut, width - cut, (spread, metric_parts),
        kept, widen(weighted), turn(applied[:, :rows]))
    rest = turn_back(rest_turned)
    right = jnp.einsum("tac,cb->tab", weighted, fock, preferred_element_type=jnp.float32)
    left_wide = jnp.pad(left[:, :rows], ((0, 0), (0, 0), (cut, 0)))
    sigma = left_wide.astype(jnp.float32) + right + rest.astype(jnp.float32)
    wide = amplitudes.astype(jnp.float32)
    weighted_wide = weighted.astype(jnp.float32)
    numer_local = jnp.sum(wide * sigma)
    denom_local = jnp.sum(wide * weighted_wide)
    numerator, denominator = sum_all((numer_local, denom_local), groups, peers, 3)
    rayleigh = numerator / denominator
    resid = sigma - rayleigh * weighted_wide
    squares, = sum_all((jnp.sum(resid * resid),), groups, peers, 4)
    return resid.astype(jnp.bfloat16), rayleigh, squares / denominator


def solution(mesh):
    placed = (P("act", "virt", None), P(), P(), P())
    return jax.shard_map(
        local,
        mesh=mesh,
        in_specs=placed,
        out_specs=(P("act", "virt", None), P(), P()),
        check_vma=False,
    )
```

```python
import functools

import jax
import jax.numpy as jnp
from jax import lax
from jax.experimental import pallas as pl
from jax.experimental.pallas import tpu as pltpu
from jax.sharding import PartitionSpec as P

MESH = pl.DeviceIdType.MESH
AHEAD = 4


def stage_kernel(first, peers, groups, pair_count, start, *refs):
    if first:
        (shift_ref, fock_ref, metric_ref, active_ref, image_ref, rows_ref,
         left_ref, back_ref, kept_ref) = refs[:9]
        scratch = refs[9:]
    else:
        fock_ref, metric_ref, kept_ref, image_ref, rows_ref, left_ref, back_ref = refs[:7]
        scratch = refs[7:]
    (held, made, row_held, row_made, sent, landed, back_sent, back_landed,
     row_sent, row_landed, row_back_sent, row_back_landed) = scratch
    group = lax.axis_index("act")
    me = lax.axis_index("virt")
    rounds, rows, width = held.shape[0], held.shape[2], held.shape[3]
    items = row_held.shape[0]
    per_step = -(-items // rounds)
    barrier = pltpu.get_barrier_semaphore()
    for step in range(1, peers):
        pl.semaphore_signal(
            barrier, inc=1, device_id=(group, lax.rem(me + step, peers)), device_id_type=MESH)
    for step in range(1, groups):
        pl.semaphore_signal(
            barrier, inc=1, device_id=(lax.rem(group + step, groups), me), device_id_type=MESH)
    pl.semaphore_wait(barrier, peers + groups - 2)

    def slab(t):
        return image_ref.at[t, :, pl.ds(start, width)]

    def forward(r, peer):
        return pltpu.make_async_remote_copy(
            src_ref=slab(r * peers + peer), dst_ref=held.at[r, me],
            send_sem=sent.at[r, peer], recv_sem=landed.at[r, me],
            device_id=(group, peer), device_id_type=MESH)

    def forward_own(r):
        return pltpu.make_async_copy(slab(r * peers + me), held.at[r, me], landed.at[r, me])

    def arrival(r, peer):
        return pltpu.make_async_remote_copy(
            src_ref=made.at[r, peer], dst_ref=held.at[r, peer],
            send_sem=sent.at[r, peer], recv_sem=landed.at[r, peer],
            device_id=(group, peer), device_id_type=MESH)

    def backward(r, peer):
        return pltpu.make_async_remote_copy(
            src_ref=made.at[r, peer], dst_ref=left_ref.at[r * peers + me],
            send_sem=back_sent.at[r, peer], recv_sem=back_landed.at[r, me],
            device_id=(group, peer), device_id_type=MESH)

    def backward_own(r):
        return pltpu.make_async_copy(made.at[r, me], left_ref.at[r * peers + me], back_landed.at[r, me])

    def back_arrival(r, peer):
        return pltpu.make_async_remote_copy(
            src_ref=made.at[r, peer], dst_ref=left_ref.at[r * peers + peer],
            send_sem=back_sent.at[r, peer], recv_sem=back_landed.at[r, peer],
            device_id=(group, peer), device_id_type=MESH)

    def row_forward(i, peer):
        return pltpu.make_async_remote_copy(
            src_ref=rows_ref.at[peer * items + i], dst_ref=row_held.at[i, group],
            send_sem=row_sent.at[i, peer], recv_sem=row_landed.at[i, group],
            device_id=(peer, me), device_id_type=MESH)

    def row_forward_own(i):
        return pltpu.make_async_copy(
            rows_ref.at[group * items + i], row_held.at[i, group], row_landed.at[i, group])

    def row_arrival(i, peer):
        return pltpu.make_async_remote_copy(
            src_ref=rows_ref.at[peer * items + i], dst_ref=row_held.at[i, peer],
            send_sem=row_sent.at[i, peer], recv_sem=row_landed.at[i, peer],
            device_id=(peer, me), device_id_type=MESH)

    def row_backward(i, peer):
        return pltpu.make_async_remote_copy(
            src_ref=row_made.at[i, peer], dst_ref=back_ref.at[group * items + i],
            send_sem=row_back_sent.at[i, peer], recv_sem=row_back_landed.at[i, group],
            device_id=(peer, me), device_id_type=MESH)

    def row_backward_own(i):
        return pltpu.make_async_copy(
            row_made.at[i, group], back_ref.at[group * items + i], row_back_landed.at[i, group])

    def row_back_arrival(i, peer):
        return pltpu.make_async_remote_copy(
            src_ref=row_made.at[i, peer], dst_ref=back_ref.at[peer * items + i],
            send_sem=row_back_sent.at[i, peer], recv_sem=row_back_landed.at[i, peer],
            device_id=(peer, me), device_id_type=MESH)

    def launch(r):
        for step in range(peers):
            peer = lax.rem(me + step, peers)

            @pl.when(r * peers + peer < pair_count)
            def _(step=step, peer=peer):
                if step == 0:
                    forward_own(r).start()
                else:
                    forward(r, peer).start()

        def launch_row(i, carry):
            row_forward_own(i).start()
            for step in range(1, groups):
                row_forward(i, lax.rem(group + step, groups)).start()
            return carry

        lax.fori_loop(jnp.minimum(r * per_step, items), jnp.minimum((r + 1) * per_step, items), launch_row, 0)

    def ahead(r, carry):
        launch(r)
        return carry

    lax.fori_loop(0, min(AHEAD, rounds), ahead, 0)

    def mix(matrix_ref, i):
        total = jnp.dot(matrix_ref[0], row_held[i, 0], preferred_element_type=jnp.float32)
        for q in range(1, groups):
            total += jnp.dot(matrix_ref[q], row_held[i, q], preferred_element_type=jnp.float32)
        return total

    def mix_row(i, carry):
        row_forward_own(i).wait()
        for step in range(1, groups):
            row_arrival(i, lax.rem(group + step, groups)).wait_recv()
        tall = row_held.shape[2]
        weighted = mix(metric_ref, i)
        if first:
            half = weighted.astype(jnp.bfloat16)
            row_made[i] = half.reshape(groups, tall, -1)
            active = mix(active_ref, i) - shift_ref[0] * (weighted - half.astype(jnp.float32))
            kept_ref[i] = active.astype(jnp.bfloat16).reshape(groups, tall, -1)
        else:
            wide = row_held.shape[3]
            kept = kept_ref[i, :, :, :wide].astype(jnp.float32)
            row_made[i, :, :, :wide] = (kept + weighted.reshape(groups, tall, wide)).astype(jnp.bfloat16)
            row_made[i, :, :, wide:] = kept_ref[i, :, :, wide:]
        row_backward_own(i).start()
        for step in range(1, groups):
            row_backward(i, lax.rem(group + step, groups)).start()
        return carry

    def body(r, carry):
        @pl.when(r + AHEAD < rounds)
        def _():
            launch(r + AHEAD)

        lax.fori_loop(jnp.minimum(r * per_step, items), jnp.minimum((r + 1) * per_step, items), mix_row, 0)

        @pl.when(r * peers + me < pair_count)
        def _():
            forward_own(r).wait()
            for step in range(1, peers):
                arrival(r, lax.rem(me + step, peers)).wait_recv()
            block = held[r].reshape(peers * rows, width)
            product = jnp.dot(fock_ref[...], block, preferred_element_type=jnp.float32)
            made[r] = product.astype(jnp.bfloat16).reshape(peers, rows, width)
            backward_own(r).start()
            for step in range(1, peers):
                backward(r, lax.rem(me + step, peers)).start()

        return carry

    lax.fori_loop(0, rounds, body, 0)

    def drain(r, carry):
        mine = r * peers + me < pair_count

        @pl.when(mine)
        def _():
            backward_own(r).wait()

        for step in range(1, peers):
            peer = lax.rem(me + step, peers)

            @pl.when(r * peers + peer < pair_count)
            def _(peer=peer):
                forward(r, peer).wait_send()
                back_arrival(r, peer).wait_recv()

            @pl.when(mine)
            def _(peer=peer):
                backward(r, peer).wait_send()

        return carry

    lax.fori_loop(0, rounds, drain, 0)

    def drain_row(i, carry):
        row_backward_own(i).wait()
        for step in range(1, groups):
            peer = lax.rem(group + step, groups)
            row_forward(i, peer).wait_send()
            row_back_arrival(i, peer).wait_recv()
            row_backward(i, peer).wait_send()
        return carry

    lax.fori_loop(0, items, drain_row, 0)


def stage(first, peers, groups, pairs, start, width, smalls, kept, image, turned):
    fock = smalls[1] if first else smalls[0]
    padded = image.shape[1]
    count, tall, row_width = turned.shape
    items = count // groups
    rounds = -(-pairs // peers)
    full = image.shape[2]
    whole = pl.BlockSpec(memory_space=pltpu.VMEM)
    anywhere = pl.BlockSpec(memory_space=pl.ANY)
    made_rows = (items, groups, tall, full)
    out_shape = [
        jax.ShapeDtypeStruct((pairs, padded, width), jnp.bfloat16),
        jax.ShapeDtypeStruct((count, tall, full), jnp.bfloat16),
    ]
    out_specs = [anywhere, anywhere]
    if first:
        in_specs = [pl.BlockSpec(memory_space=pltpu.SMEM)] + [whole] * 3
        out_shape.append(jax.ShapeDtypeStruct(made_rows, jnp.bfloat16))
        out_specs.append(whole)
        operands = smalls
    else:
        in_specs = [whole] * 3
        operands = (*smalls, kept)
    dma = pltpu.SemaphoreType.DMA
    return pl.pallas_call(
        functools.partial(stage_kernel, first, peers, groups, pairs, start),
        out_shape=out_shape,
        in_specs=in_specs + [anywhere] * 2,
        out_specs=out_specs,
        scratch_shapes=[
            pltpu.VMEM((rounds, peers, padded, width), jnp.bfloat16),
            pltpu.VMEM((rounds, peers, padded, width), jnp.bfloat16),
            pltpu.VMEM((items, groups, tall, row_width), jnp.bfloat16),
            pltpu.VMEM(made_rows, jnp.bfloat16),
            dma((rounds, peers)), dma((rounds, peers)), dma((rounds, peers)), dma((rounds, peers)),
            dma((items, groups)), dma((items, groups)), dma((items, groups)), dma((items, groups)),
        ],
        compiler_params=pltpu.CompilerParams(
            collective_id=1 if first else 2, has_side_effects=True, vmem_limit_bytes=60 * 2**20),
        cost_estimate=pl.CostEstimate(
            flops=2 * pairs * fock.size * width, bytes_accessed=400 * 2**20, transcendentals=0),
    )(*operands, image, turned)


def finish_kernel(groups, peers, fock_ref, trial_ref, image_ref, left_ref, rest_ref, out_ref, stats_ref,
                  trial, image, left, rest, sigma, part, slots, loaded, stored, sent, landed):
    group, me = lax.axis_index("act"), lax.axis_index("virt")
    count = groups * peers
    mine = group * peers + me
    barrier = pltpu.get_barrier_semaphore()
    chunks = loaded.shape[1]
    depth = trial.shape[0] // chunks
    rows, width = trial.shape[1], trial.shape[2]
    tail = left.shape[2]
    cut = width - tail

    def span(c):
        return pl.ds(c * depth, depth)

    def load(c, which):
        source, target = ((trial_ref, trial), (image_ref, image), (left_ref, left), (rest_ref, rest))[which]
        return pltpu.make_async_copy(source.at[span(c)], target.at[span(c)], loaded.at[which, c])

    def load_all(c, carry):
        for which in range(4):
            load(c, which).start()
        return carry

    lax.fori_loop(0, chunks, load_all, 0)

    def target(step):
        other = lax.rem(mine + step, count)
        return other, (other // peers, lax.rem(other, peers))

    def greet(step, carry):
        pl.semaphore_signal(barrier, inc=1, device_id=target(step)[1], device_id_type=MESH)
        return carry

    lax.fori_loop(1, count, greet, 0)

    def product(c, carry):
        numer, denom = carry
        for which in range(4):
            load(c, which).wait()
        own = image[span(c)].reshape(depth * rows, width)
        total = jnp.dot(own, fock_ref[...], preferred_element_type=jnp.float32)
        total += rest[span(c)].reshape(depth * rows, width).astype(jnp.float32)
        last = total[:, cut:] + left[span(c)].reshape(depth * rows, tail).astype(jnp.float32)
        total = jnp.concatenate([total[:, :cut], last], axis=1)
        sigma[span(c)] = total.reshape(depth, rows, width)
        wide = trial[span(c)].reshape(depth * rows, width).astype(jnp.float32)
        numer += jnp.sum(wide * total, axis=0, keepdims=True)
        denom += jnp.sum(wide * own.astype(jnp.float32), axis=0, keepdims=True)
        return numer, denom

    zero = jnp.zeros((1, width), jnp.float32)
    numer, denom = lax.fori_loop(0, chunks, product, (zero, zero))
    pl.semaphore_wait(barrier, count - 1)

    def sum_all(phase, value):
        part[phase] = value

        def copy(step, slot):
            other, place = target(step)
            return pltpu.make_async_remote_copy(
                src_ref=part.at[phase], dst_ref=slots.at[phase, slot],
                send_sem=sent.at[phase, other], recv_sem=landed.at[phase, slot],
                device_id=place, device_id_type=MESH)

        def send(step, carry):
            copy(step, mine).start()
            return carry

        lax.fori_loop(1, count, send, 0)
        slots[phase, mine] = value

        def receive(step, carry):
            copy(step, target(step)[0]).wait_recv()
            return carry

        lax.fori_loop(1, count, receive, 0)

        def finish(step, carry):
            copy(step, mine).wait_send()
            return carry

        lax.fori_loop(1, count, finish, 0)
        return jnp.sum(slots[phase], axis=0)

    row = lax.broadcasted_iota(jnp.int32, (8, 128), 0)
    numer_one = jnp.sum(numer, axis=1, keepdims=True)
    denom_one = jnp.sum(denom, axis=1, keepdims=True)
    sums = sum_all(0, jnp.where(row == 0, numer_one, denom_one))
    denominator = sums[1:2, 0:1]
    rayleigh = sums[0:1, 0:1] / denominator

    def store(c):
        return pltpu.make_async_copy(rest.at[span(c)], out_ref.at[span(c)], stored.at[c])

    def residual(c, squares):
        own = image[span(c)].reshape(depth * rows, width).astype(jnp.float32)
        resid = sigma[span(c)].reshape(depth * rows, width) - rayleigh * own
        rest[span(c)] = resid.astype(jnp.bfloat16).reshape(depth, rows, width)
        store(c).start()
        return squares + jnp.sum(resid * resid, axis=0, keepdims=True)

    squares = lax.fori_loop(0, chunks, residual, zero)
    square_one = jnp.sum(squares, axis=1, keepdims=True)
    norms = sum_all(1, jnp.broadcast_to(square_one, (8, 128)))
    stats_ref[...] = jnp.where(row == 0, rayleigh, norms / denominator)

    def drain(c, carry):
        store(c).wait()
        return carry

    lax.fori_loop(0, chunks, drain, 0)


def finish(groups, peers, fock, trial, image, left, rest):
    pairs, rows, width = trial.shape
    depth = next(d for d in (5, 4, 2, 1) if pairs % d == 0)
    chunks = pairs // depth
    whole = pl.BlockSpec(memory_space=pltpu.VMEM)
    anywhere = pl.BlockSpec(memory_space=pl.ANY)
    dma = pltpu.SemaphoreType.DMA
    count = groups * peers
    return pl.pallas_call(
        functools.partial(finish_kernel, groups, peers),
        out_shape=[
            jax.ShapeDtypeStruct((pairs, rows, width), jnp.bfloat16),
            jax.ShapeDtypeStruct((8, 128), jnp.float32),
        ],
        in_specs=[whole] + [anywhere] * 4,
        out_specs=[anywhere, whole],
        scratch_shapes=[
            pltpu.VMEM((pairs, rows, width), jnp.bfloat16),
            pltpu.VMEM((pairs, rows, width), jnp.bfloat16),
            pltpu.VMEM((pairs, rows, left.shape[2]), jnp.bfloat16),
            pltpu.VMEM((pairs, rows, width), jnp.bfloat16),
            pltpu.VMEM((pairs, rows, width), jnp.float32),
            pltpu.VMEM((2, 8, 128), jnp.float32),
            pltpu.VMEM((2, count, 8, 128), jnp.float32),
            dma((4, chunks)), dma((chunks,)), dma((2, count)), dma((2, count)),
        ],
        compiler_params=pltpu.CompilerParams(
            collective_id=3, has_side_effects=True, vmem_limit_bytes=63 * 2**20),
    )(fock, trial, image, left, rest)


def local(amplitudes, virtual_fock_block, metric, active_block):
    pairs, rows, width = amplitudes.shape
    peers, groups = lax.axis_size("virt"), lax.axis_size("act")
    fock = virtual_fock_block
    padded = -(-rows // 16) * 16
    tall = -(-pairs // 8) * 8
    cut = (3 * width // 5) // 128 * 128

    def widen(array):
        if padded == rows:
            return array
        return jnp.pad(array, ((0, 0), (0, padded - rows), (0, 0)))

    def turn(array):
        return jnp.pad(jnp.transpose(array, (1, 0, 2)), ((0, 0), (0, tall - pairs), (0, 0)))

    def turn_back(array):
        return jnp.transpose(array, (1, 0, 2))

    def pair_matrix(array):
        room = tall - pairs
        spread = jnp.pad(
            array.reshape(groups, pairs, groups, pairs), ((0, 0), (0, room), (0, 0), (0, room)))
        return jnp.transpose(spread, (2, 0, 1, 3)).reshape(groups, groups * tall, tall)

    spread = fock
    if padded != rows:
        room = padded - rows
        spread = jnp.pad(
            fock.reshape(peers, rows, peers, rows), ((0, 0), (0, room), (0, 0), (0, room))
        ).reshape(peers * padded, peers * padded)
    metric_parts, active_parts = pair_matrix(metric), pair_matrix(active_block)
    at = lax.broadcasted_iota(jnp.int32, fock.shape, 0)
    across = lax.broadcasted_iota(jnp.int32, fock.shape, 1)
    shift = (2.0 / width) * jnp.sum(jnp.where(at == across, fock.astype(jnp.float32), 0.0))
    trial = widen(amplitudes)
    applied, weighted_turned, kept = stage(
        True, peers, groups, pairs, 0, cut, (shift.reshape(1), spread, metric_parts, active_parts),
        None, trial, turn(amplitudes))
    weighted = widen(turn_back(weighted_turned))
    left, rest_turned = stage(
        False, peers, groups, pairs, cut, width - cut, (spread, metric_parts),
        kept, weighted, turn(applied[:, :rows]))
    rest = widen(turn_back(rest_turned))
    resid, stats = finish(groups, peers, fock, trial, weighted, left, rest)
    return resid[:, :rows], stats[0, 0], stats[1, 0]


def solution(mesh):
    placed = (P("act", "virt", None), P(), P(), P())
    return jax.shard_map(
        local,
        mesh=mesh,
        in_specs=placed,
        out_specs=(P("act", "virt", None), P(), P()),
        check_vma=False,
    )
```

```python
import functools

import jax
import jax.numpy as jnp
from jax import lax
from jax.experimental import pallas as pl
from jax.experimental.pallas import tpu as pltpu
from jax.sharding import PartitionSpec as P

MESH = pl.DeviceIdType.MESH
AHEAD = 4


def stage_kernel(first, peers, groups, pair_count, start, *refs):
    if first:
        (shift_ref, fock_ref, metric_ref, active_ref, image_ref, rows_ref,
         left_ref, back_ref, kept_ref, early_ref) = refs[:10]
        *scratch, early_sent, early_landed = refs[10:]
    else:
        fock_ref, metric_ref, kept_ref, image_ref, rows_ref, left_ref, back_ref = refs[:7]
        scratch = refs[7:]
    (held, made, row_held, row_made, sent, landed, back_sent, back_landed,
     row_sent, row_landed, row_back_sent, row_back_landed) = scratch
    group = lax.axis_index("act")
    me = lax.axis_index("virt")
    rounds, rows, width = held.shape[0], held.shape[2], held.shape[3]
    items = row_held.shape[0]
    per_step = -(-items // rounds)
    barrier = pltpu.get_barrier_semaphore()
    for step in range(1, peers):
        pl.semaphore_signal(
            barrier, inc=1, device_id=(group, lax.rem(me + step, peers)), device_id_type=MESH)
    for step in range(1, groups):
        pl.semaphore_signal(
            barrier, inc=1, device_id=(lax.rem(group + step, groups), me), device_id_type=MESH)
    pl.semaphore_wait(barrier, peers + groups - 2)

    whole_rounds = pair_count // peers
    spare = pair_count % peers
    stride = peers // spare if spare and peers % spare == 0 else 1

    def pair_of(r, owner):
        return r * peers + owner - (r // whole_rounds) * (owner - owner // stride)

    def owns(r, owner):
        return (r // whole_rounds) * peers * lax.rem(owner, stride) + pair_of(r, owner) < pair_count

    def slab(t):
        return image_ref.at[t, :, pl.ds(start, width)]

    def forward(r, peer):
        return pltpu.make_async_remote_copy(
            src_ref=slab(pair_of(r, peer)), dst_ref=held.at[r, me],
            send_sem=sent.at[r, peer], recv_sem=landed.at[r, me],
            device_id=(group, peer), device_id_type=MESH)

    def forward_own(r):
        return pltpu.make_async_copy(slab(pair_of(r, me)), held.at[r, me], landed.at[r, me])

    def arrival(r, peer):
        return pltpu.make_async_remote_copy(
            src_ref=made.at[r, peer], dst_ref=held.at[r, peer],
            send_sem=sent.at[r, peer], recv_sem=landed.at[r, peer],
            device_id=(group, peer), device_id_type=MESH)

    def backward(r, peer):
        return pltpu.make_async_remote_copy(
            src_ref=made.at[r, peer], dst_ref=left_ref.at[pair_of(r, me)],
            send_sem=back_sent.at[r, peer], recv_sem=back_landed.at[r, me],
            device_id=(group, peer), device_id_type=MESH)

    def backward_own(r):
        return pltpu.make_async_copy(made.at[r, me], left_ref.at[pair_of(r, me)], back_landed.at[r, me])

    def back_arrival(r, peer):
        return pltpu.make_async_remote_copy(
            src_ref=made.at[r, peer], dst_ref=left_ref.at[pair_of(r, peer)],
            send_sem=back_sent.at[r, peer], recv_sem=back_landed.at[r, peer],
            device_id=(group, peer), device_id_type=MESH)

    def row_forward(i, peer):
        return pltpu.make_async_remote_copy(
            src_ref=rows_ref.at[peer * items + i], dst_ref=row_held.at[i, group],
            send_sem=row_sent.at[i, peer], recv_sem=row_landed.at[i, group],
            device_id=(peer, me), device_id_type=MESH)

    def row_forward_own(i):
        return pltpu.make_async_copy(
            rows_ref.at[group * items + i], row_held.at[i, group], row_landed.at[i, group])

    def row_arrival(i, peer):
        return pltpu.make_async_remote_copy(
            src_ref=rows_ref.at[peer * items + i], dst_ref=row_held.at[i, peer],
            send_sem=row_sent.at[i, peer], recv_sem=row_landed.at[i, peer],
            device_id=(peer, me), device_id_type=MESH)

    def row_backward(i, peer):
        return pltpu.make_async_remote_copy(
            src_ref=row_made.at[i, peer], dst_ref=back_ref.at[group * items + i],
            send_sem=row_back_sent.at[i, peer], recv_sem=row_back_landed.at[i, group],
            device_id=(peer, me), device_id_type=MESH)

    def row_backward_own(i):
        return pltpu.make_async_copy(
            row_made.at[i, group], back_ref.at[group * items + i], row_back_landed.at[i, group])

    def row_back_arrival(i, peer):
        return pltpu.make_async_remote_copy(
            src_ref=row_made.at[i, peer], dst_ref=back_ref.at[peer * items + i],
            send_sem=row_back_sent.at[i, peer], recv_sem=row_back_landed.at[i, peer],
            device_id=(peer, me), device_id_type=MESH)

    if first:
        early_width = early_ref.shape[2]
        early_columns = pl.ds(kept_ref.shape[3] - early_width, early_width)

        def early(i, peer):
            return pltpu.make_async_remote_copy(
                src_ref=kept_ref.at[i, peer, :, early_columns], dst_ref=early_ref.at[group * items + i],
                send_sem=early_sent.at[i, peer], recv_sem=early_landed.at[i, group],
                device_id=(peer, me), device_id_type=MESH)

        def early_own(i):
            return pltpu.make_async_copy(
                kept_ref.at[i, group, :, early_columns], early_ref.at[group * items + i],
                early_landed.at[i, group])

        def early_arrival(i, peer):
            return pltpu.make_async_remote_copy(
                src_ref=kept_ref.at[i, peer, :, early_columns], dst_ref=early_ref.at[peer * items + i],
                send_sem=early_sent.at[i, peer], recv_sem=early_landed.at[i, peer],
                device_id=(peer, me), device_id_type=MESH)

    def launch(r):
        for step in range(peers):
            peer = lax.rem(me + step, peers)

            @pl.when(owns(r, peer))
            def _(step=step, peer=peer):
                if step == 0:
                    forward_own(r).start()
                else:
                    forward(r, peer).start()

        def launch_row(i, carry):
            row_forward_own(i).start()
            for step in range(1, groups):
                row_forward(i, lax.rem(group + step, groups)).start()
            return carry

        lax.fori_loop(jnp.minimum(r * per_step, items), jnp.minimum((r + 1) * per_step, items), launch_row, 0)

    def ahead(r, carry):
        launch(r)
        return carry

    lax.fori_loop(0, min(AHEAD, rounds), ahead, 0)

    def mix(matrix_ref, i):
        total = jnp.dot(matrix_ref[0], row_held[i, 0], preferred_element_type=jnp.float32)
        for q in range(1, groups):
            total += jnp.dot(matrix_ref[q], row_held[i, q], preferred_element_type=jnp.float32)
        return total.reshape(groups, -1, total.shape[1])[:, :row_held.shape[2]]

    def mix_row(i, carry):
        row_forward_own(i).wait()
        for step in range(1, groups):
            row_arrival(i, lax.rem(group + step, groups)).wait_recv()
        weighted = mix(metric_ref, i)
        if first:
            half = weighted.astype(jnp.bfloat16)
            row_made[i] = half
            active = mix(active_ref, i) - shift_ref[0] * (weighted - half.astype(jnp.float32))
            kept_ref[i] = active.astype(jnp.bfloat16)
            early_own(i).start()
            for step in range(1, groups):
                early(i, lax.rem(group + step, groups)).start()
        else:
            wide, part = row_held.shape[3], row_made.shape[3]
            kept = kept_ref[i, :, :, :wide].astype(jnp.float32)
            row_made[i, :, :, :wide] = (kept + weighted).astype(jnp.bfloat16)
            if part > wide:
                row_made[i, :, :, wide:] = kept_ref[i, :, :, wide:part]
        row_backward_own(i).start()
        for step in range(1, groups):
            row_backward(i, lax.rem(group + step, groups)).start()
        return carry

    def body(r, carry):
        @pl.when(r + AHEAD < rounds)
        def _():
            launch(r + AHEAD)

        lax.fori_loop(jnp.minimum(r * per_step, items), jnp.minimum((r + 1) * per_step, items), mix_row, 0)

        @pl.when(owns(r, me))
        def _():
            forward_own(r).wait()
            for step in range(1, peers):
                arrival(r, lax.rem(me + step, peers)).wait_recv()
            block = held[r].reshape(peers * rows, width)
            product = jnp.dot(fock_ref[...], block, preferred_element_type=jnp.float32)
            made[r] = product.astype(jnp.bfloat16).reshape(peers, rows, width)
            backward_own(r).start()
            for step in range(1, peers):
                backward(r, lax.rem(me + step, peers)).start()

        return carry

    lax.fori_loop(0, rounds, body, 0)

    def drain(r, carry):
        mine = owns(r, me)

        @pl.when(mine)
        def _():
            backward_own(r).wait()

        for step in range(1, peers):
            peer = lax.rem(me + step, peers)

            @pl.when(owns(r, peer))
            def _(peer=peer):
                forward(r, peer).wait_send()
                back_arrival(r, peer).wait_recv()

            @pl.when(mine)
            def _(peer=peer):
                backward(r, peer).wait_send()

        return carry

    lax.fori_loop(0, rounds, drain, 0)

    def drain_row(i, carry):
        row_backward_own(i).wait()
        for step in range(1, groups):
            peer = lax.rem(group + step, groups)
            row_forward(i, peer).wait_send()
            row_back_arrival(i, peer).wait_recv()
            row_backward(i, peer).wait_send()
            if first:
                early_arrival(i, peer).wait_recv()
                early(i, peer).wait_send()
        if first:
            early_own(i).wait()
        return carry

    lax.fori_loop(0, items, drain_row, 0)


def stage(first, peers, groups, pairs, start, width, tail, smalls, kept, image, turned):
    fock = smalls[1] if first else smalls[0]
    padded = image.shape[1]
    count, tall, row_width = turned.shape
    items = count // groups
    rounds = -(-pairs // peers)
    full = image.shape[2]
    whole = pl.BlockSpec(memory_space=pltpu.VMEM)
    anywhere = pl.BlockSpec(memory_space=pl.ANY)
    kept_rows = (items, groups, tall, full)
    made_width = full if first else full - tail
    out_shape = [
        jax.ShapeDtypeStruct((pairs, padded, width), jnp.bfloat16),
        jax.ShapeDtypeStruct((count, tall, made_width), jnp.bfloat16),
    ]
    out_specs = [anywhere, anywhere]
    if first:
        in_specs = [pl.BlockSpec(memory_space=pltpu.SMEM)] + [whole] * 3
        out_shape.append(jax.ShapeDtypeStruct(kept_rows, jnp.bfloat16))
        out_shape.append(jax.ShapeDtypeStruct((count, tall, tail), jnp.bfloat16))
        out_specs += [whole, anywhere]
        operands = smalls
    else:
        in_specs = [whole] * 3
        operands = (*smalls, kept)
    dma = pltpu.SemaphoreType.DMA
    return pl.pallas_call(
        functools.partial(stage_kernel, first, peers, groups, pairs, start),
        out_shape=out_shape,
        in_specs=in_specs + [anywhere] * 2,
        out_specs=out_specs,
        scratch_shapes=[
            pltpu.VMEM((rounds, peers, padded, width), jnp.bfloat16),
            pltpu.VMEM((rounds, peers, padded, width), jnp.bfloat16),
            pltpu.VMEM((items, groups, tall, row_width), jnp.bfloat16),
            pltpu.VMEM((items, groups, tall, made_width), jnp.bfloat16),
            dma((rounds, peers)), dma((rounds, peers)), dma((rounds, peers)), dma((rounds, peers)),
            dma((items, groups)), dma((items, groups)), dma((items, groups)), dma((items, groups)),
        ] + [dma((items, groups))] * (2 if first else 0),
        compiler_params=pltpu.CompilerParams(
            collective_id=1 if first else 2, has_side_effects=True, vmem_limit_bytes=60 * 2**20),
        cost_estimate=pl.CostEstimate(
            flops=2 * pairs * fock.size * width, bytes_accessed=400 * 2**20, transcendentals=0),
    )(*operands, image, turned)


def finish_kernel(groups, peers, fock_ref, trial_ref, image_ref, left_ref, rest_ref, early_ref, out_ref, stats_ref,
                  trial, image, left, rest, sigma, part, slots, loaded, stored, sent, landed):
    group, me = lax.axis_index("act"), lax.axis_index("virt")
    count = groups * peers
    mine = group * peers + me
    barrier = pltpu.get_barrier_semaphore()
    chunks = loaded.shape[1]
    depth = trial.shape[0] // chunks
    rows, width = trial.shape[1], trial.shape[2]
    tail = left.shape[2]
    cut = width - tail

    def span(c):
        return pl.ds(c * depth, depth)

    def load(c, which):
        source, target = ((trial_ref, trial), (image_ref, image), (left_ref, left))[which]
        return pltpu.make_async_copy(source.at[span(c)], target.at[span(c)], loaded.at[which, c])

    def load_rest(c):
        head = rest_ref.shape[2]
        return (
            pltpu.make_async_copy(
                rest_ref.at[span(c)], rest.at[span(c), :, pl.ds(0, head)], loaded.at[3, c]),
            pltpu.make_async_copy(
                early_ref.at[span(c)], rest.at[span(c), :, pl.ds(head, width - head)], loaded.at[4, c]))

    def load_all(c, carry):
        for which in range(3):
            load(c, which).start()
        for copy in load_rest(c):
            copy.start()
        return carry

    lax.fori_loop(0, chunks, load_all, 0)

    def target(step):
        other = lax.rem(mine + step, count)
        return other, (other // peers, lax.rem(other, peers))

    def greet(step, carry):
        pl.semaphore_signal(barrier, inc=1, device_id=target(step)[1], device_id_type=MESH)
        return carry

    lax.fori_loop(1, count, greet, 0)

    def product(c, carry):
        numer, denom = carry
        for which in range(3):
            load(c, which).wait()
        for copy in load_rest(c):
            copy.wait()
        own = image[span(c)].reshape(depth * rows, width)
        total = jnp.dot(own, fock_ref[...], preferred_element_type=jnp.float32)
        total += rest[span(c)].reshape(depth * rows, width).astype(jnp.float32)
        last = total[:, cut:] + left[span(c)].reshape(depth * rows, tail).astype(jnp.float32)
        total = jnp.concatenate([total[:, :cut], last], axis=1)
        sigma[span(c)] = total.reshape(depth, rows, width)
        wide = trial[span(c)].reshape(depth * rows, width).astype(jnp.float32)
        numer += jnp.sum(wide * total, axis=0, keepdims=True)
        denom += jnp.sum(wide * own.astype(jnp.float32), axis=0, keepdims=True)
        return numer, denom

    zero = jnp.zeros((1, width), jnp.float32)
    numer, denom = lax.fori_loop(0, chunks, product, (zero, zero))
    pl.semaphore_wait(barrier, count - 1)

    def sum_all(phase, value):
        part[phase] = value

        def copy(step, slot):
            other, place = target(step)
            return pltpu.make_async_remote_copy(
                src_ref=part.at[phase], dst_ref=slots.at[phase, slot],
                send_sem=sent.at[phase, other], recv_sem=landed.at[phase, slot],
                device_id=place, device_id_type=MESH)

        def send(step, carry):
            copy(step, mine).start()
            return carry

        lax.fori_loop(1, count, send, 0)
        slots[phase, mine] = value

        def receive(step, carry):
            copy(step, target(step)[0]).wait_recv()
            return carry

        lax.fori_loop(1, count, receive, 0)

        def finish(step, carry):
            copy(step, mine).wait_send()
            return carry

        lax.fori_loop(1, count, finish, 0)
        return jnp.sum(slots[phase], axis=0)

    row = lax.broadcasted_iota(jnp.int32, (8, 128), 0)
    numer_one = jnp.sum(numer, axis=1, keepdims=True)
    denom_one = jnp.sum(denom, axis=1, keepdims=True)
    sums = sum_all(0, jnp.where(row == 0, numer_one, denom_one))
    denominator = sums[1:2, 0:1]
    rayleigh = sums[0:1, 0:1] / denominator

    def store(c):
        return pltpu.make_async_copy(rest.at[span(c)], out_ref.at[span(c)], stored.at[c])

    def residual(c, squares):
        own = image[span(c)].reshape(depth * rows, width).astype(jnp.float32)
        resid = sigma[span(c)].reshape(depth * rows, width) - rayleigh * own
        rest[span(c)] = resid.astype(jnp.bfloat16).reshape(depth, rows, width)
        store(c).start()
        return squares + jnp.sum(resid * resid, axis=0, keepdims=True)

    squares = lax.fori_loop(0, chunks, residual, zero)
    square_one = jnp.sum(squares, axis=1, keepdims=True)
    norms = sum_all(1, jnp.broadcast_to(square_one, (8, 128)))
    stats_ref[...] = jnp.where(row == 0, rayleigh, norms / denominator)

    def drain(c, carry):
        store(c).wait()
        return carry

    lax.fori_loop(0, chunks, drain, 0)


def finish(groups, peers, fock, trial, image, left, rest, early):
    pairs, rows, width = trial.shape
    depth = next(d for d in (5, 4, 2, 1) if pairs % d == 0)
    chunks = pairs // depth
    whole = pl.BlockSpec(memory_space=pltpu.VMEM)
    anywhere = pl.BlockSpec(memory_space=pl.ANY)
    dma = pltpu.SemaphoreType.DMA
    count = groups * peers
    return pl.pallas_call(
        functools.partial(finish_kernel, groups, peers),
        out_shape=[
            jax.ShapeDtypeStruct((pairs, rows, width), jnp.bfloat16),
            jax.ShapeDtypeStruct((8, 128), jnp.float32),
        ],
        in_specs=[whole] + [anywhere] * 5,
        out_specs=[anywhere, whole],
        scratch_shapes=[
            pltpu.VMEM((pairs, rows, width), jnp.bfloat16),
            pltpu.VMEM((pairs, rows, width), jnp.bfloat16),
            pltpu.VMEM((pairs, rows, left.shape[2]), jnp.bfloat16),
            pltpu.VMEM((pairs, rows, width), jnp.bfloat16),
            pltpu.VMEM((pairs, rows, width), jnp.float32),
            pltpu.VMEM((2, 8, 128), jnp.float32),
            pltpu.VMEM((2, count, 8, 128), jnp.float32),
            dma((5, chunks)), dma((chunks,)), dma((2, count)), dma((2, count)),
        ],
        compiler_params=pltpu.CompilerParams(
            collective_id=3, has_side_effects=True, vmem_limit_bytes=63 * 2**20),
    )(fock, trial, image, left, rest, early)


def local(amplitudes, virtual_fock_block, metric, active_block):
    pairs, rows, width = amplitudes.shape
    peers, groups = lax.axis_size("virt"), lax.axis_size("act")
    fock = virtual_fock_block
    padded = -(-rows // 16) * 16
    room = -pairs % 8
    cut = (3 * width // 5) // 128 * 128

    def widen(array):
        if padded == rows:
            return array
        return jnp.pad(array, ((0, 0), (0, padded - rows), (0, 0)))

    def turn(array):
        return jnp.transpose(array, (1, 0, 2))

    def turn_back(array):
        return jnp.transpose(array, (1, 0, 2))

    def pair_matrix(array):
        spread = jnp.pad(array.reshape(groups, pairs, groups, pairs), ((0, 0), (0, room), (0, 0), (0, 0)))
        return jnp.transpose(spread, (2, 0, 1, 3)).reshape(groups, groups * (pairs + room), pairs)

    spread = fock
    if padded != rows:
        gap = padded - rows
        spread = jnp.pad(
            fock.reshape(peers, rows, peers, rows), ((0, 0), (0, gap), (0, 0), (0, gap))
        ).reshape(peers * padded, peers * padded)
    metric_parts, active_parts = pair_matrix(metric), pair_matrix(active_block)
    at = lax.broadcasted_iota(jnp.int32, fock.shape, 0)
    across = lax.broadcasted_iota(jnp.int32, fock.shape, 1)
    shift = (2.0 / width) * jnp.sum(jnp.where(at == across, fock.astype(jnp.float32), 0.0))
    trial = widen(amplitudes)
    tail = min(128, width - cut)
    applied, weighted_turned, kept, early_turned = stage(
        True, peers, groups, pairs, 0, cut, tail, (shift.reshape(1), spread, metric_parts, active_parts),
        None, trial, turn(amplitudes))
    weighted = widen(turn_back(weighted_turned))
    left, rest_turned = stage(
        False, peers, groups, pairs, cut, width - cut, tail, (spread, metric_parts),
        kept, weighted, turn(applied[:, :rows]))
    rest = widen(turn_back(rest_turned))
    early = widen(turn_back(early_turned))
    resid, stats = finish(groups, peers, fock, trial, weighted, left, rest, early)
    return resid[:, :rows], stats[0, 0], stats[1, 0]


def solution(mesh):
    placed = (P("act", "virt", None), P(), P(), P())
    return jax.shard_map(
        local,
        mesh=mesh,
        in_specs=placed,
        out_specs=(P("act", "virt", None), P(), P()),
        check_vma=False,
    )
```
